32 devices in a mesh: seq: 4 (over z), grp: 8 (over y, x, core).
Axes of the slice: x: 2, y: 2, z: 4, core: 2. Of those that a mesh axis runs over, the one named last changes fastest.
Arguments:
- hidden_in: bfloat16 [8, 2048, 1024], P('grp', 'seq'), may hold values from -64 to 64, as said below
- lengths: int32 [8], P('grp'), may hold values from 256 to 2048
- project_weight: bfloat16 [1024, 3072], replicated, may hold values from -0.1875 to 0.1875
- output_weight: bfloat16 [1024, 1024], replicated, may hold values from -0.1875 to 0.1875
- first_gain: float32 [1024], replicated, may hold values from 0.5 to 1.5
- first_shift: float32 [1024], replicated, may hold values from -3 to 3
- up_weight: bfloat16 [1024, 4096], P('grp'), may hold values from -0.1875 to 0.1875
- down_weight: bfloat16 [1024, 4096], P('grp'), may hold values from -0.09375 to 0.09375
- second_gain: float32 [1024], replicated, may hold values from 0.5 to 1.5
- second_shift: float32 [1024], replicated, may hold values from -3 to 3
- queries: float32 [64, 1024], P('grp'), may hold values from -6 to 6
- positive: int32 [64], P('grp'), may hold values from 0 to 7
Outputs:
- hidden_out: bfloat16 [8, 2048, 1024], P('grp', 'seq')
- embeddings: float32 [8, 1024], P('grp')
- query_loss: float32 [64], P('grp')
The draws below stay inside these ranges and needn't reach their ends.
Inputs may be any that keep to these rules, and one draw needn't show every extreme that they name: `hidden_in`: activations.
All inputs are finite; a program needn't handle non-finite values.
Results may differ from the reference program's by a relative error of at most 0.0076.
Values may be sent and summed in bfloat16 or wider, within the bound.
A program may use at most 192 MiB of HBM per device.

```python
import math
import jax
import jax.numpy as jnp
from jax import lax

D = 1024
HEADS = 16
HEAD_DIM = 64
FF = 4096
LEN = 2048
PASSAGES = 8
QUERIES = 64


def draw_hidden_in(key, part):
    base = jnp.clip(jax.random.normal(key, (PASSAGES, LEN, D), jnp.float32), -6.0, 6.0)
    return base.astype(jnp.bfloat16)


def plant(drawn, own_key, least, high):
    spot = [jax.random.randint(jax.random.fold_in(own_key, axis), (), 0, length) for axis, length in enumerate(drawn.shape)]
    main_axis = drawn.shape.index(max(drawn.shape))
    neighbour = spot[:main_axis] + [(spot[main_axis] + 1) % drawn.shape[main_axis]] + spot[main_axis + 1:]
    return drawn.at[tuple(spot)].set(least).at[tuple(neighbour)].set(high)


def shard_levels(stream_key, dims, shards, low, top_value):
    def one(position, parts):
        draws = jax.random.uniform(jax.random.fold_in(jax.random.fold_in(stream_key, 6), position), (parts,), jnp.float32, low / len(shards), top_value / len(shards))
        return jnp.repeat(jnp.exp(draws), dims[position] // parts).reshape((-1,) + (1,) * (len(dims) - position - 1))

    factor_of = one(*shards[0])
    for cut in shards[1:]:
        factor_of = factor_of * one(*cut)
    return factor_of


def bell_draw(stream_key, dims, width, most, shards=(), kind=jnp.bfloat16):
    level = shard_levels(stream_key, dims, shards, -0.22, 0.18) if shards else 1.0
    values = jax.random.normal(stream_key, dims, jnp.float32) * width * level
    return jnp.minimum(jnp.maximum(values, -most), most).astype(kind)


def setup_inputs(seed: int = 0) -> dict:
    arg_keys = jax.random.split(jax.random.key(seed), 13)
    hidden_in = draw_hidden_in(jax.random.fold_in(arg_keys[12], 71), 0)
    lengths = plant(jax.random.randint(arg_keys[1], (PASSAGES,), LEN // 8, LEN + 1), jax.random.fold_in(arg_keys[1], 1), LEN // 8, LEN).astype(jnp.int32)
    project_weight = bell_draw(arg_keys[2], (D, 3 * D), D ** -0.5, 0.1875)
    output_weight = bell_draw(arg_keys[3], (D, D), D ** -0.5, 0.1875)
    first_gain = jnp.clip(1.0 + 0.1 * jax.random.normal(arg_keys[4], (D,), jnp.float32), 0.5, 1.5)
    first_shift = bell_draw(arg_keys[5], (D,), 0.5, 3.0, (), jnp.float32)
    up_weight = bell_draw(arg_keys[6], (D, FF), D ** -0.5, 0.1875, ((0, 8),))
    down_weight = bell_draw(arg_keys[7], (D, FF), FF ** -0.5, 0.09375, ((0, 8),))
    second_gain = jnp.clip(1.0 + 0.1 * jax.random.normal(arg_keys[8], (D,), jnp.float32), 0.5, 1.5)
    second_shift = bell_draw(arg_keys[9], (D,), 0.5, 3.0, (), jnp.float32)
    queries = bell_draw(arg_keys[10], (QUERIES, D), 1.0, 6.0, ((0, 8),), jnp.float32)
    positive = plant(jax.random.randint(arg_keys[11], (QUERIES,), 0, PASSAGES), jax.random.fold_in(arg_keys[11], 1), 0, PASSAGES - 1).astype(jnp.int32)
    return {"hidden_in": hidden_in, "lengths": lengths, "project_weight": project_weight, "output_weight": output_weight, "first_gain": first_gain, "first_shift": first_shift, "up_weight": up_weight, "down_weight": down_weight, "second_gain": second_gain, "second_shift": second_shift, "queries": queries, "positive": positive}


def layer_norm(values, gain, shift):
    average = lax.optimization_barrier(jnp.mean(values, axis=-1, keepdims=True))
    centred = values - average
    variance = lax.optimization_barrier(jnp.mean(centred * centred, axis=-1, keepdims=True))
    return centred * lax.rsqrt(variance + 1e-05) * gain + shift

def attend(projected, length):
    block = min(1024, LEN)
    query_all = projected[:, :D].reshape(LEN, HEADS, HEAD_DIM).astype(jnp.float32)
    key_all = projected[:, D:2 * D].reshape(LEN, HEADS, HEAD_DIM).astype(jnp.float32)
    value_all = projected[:, 2 * D:].reshape(LEN, HEADS, HEAD_DIM).astype(jnp.float32)
    key_valid = jnp.arange(LEN, dtype=jnp.int32) < length
    scale = 1.0 / math.sqrt(HEAD_DIM)

    def one_block(index):
        query_rows = lax.dynamic_slice_in_dim(query_all, (index * block).astype(jnp.int32), block, 0)
        scores = jnp.einsum('qhd,khd->hqk', query_rows, key_all) * scale
        scores = jnp.where(key_valid[None, None, :], scores, -jnp.inf)
        highest = lax.optimization_barrier(jnp.max(scores, axis=-1, keepdims=True))
        expo = jnp.exp(scores - highest)
        probs = (expo / lax.optimization_barrier(jnp.sum(expo, axis=-1, keepdims=True))).astype(jnp.bfloat16)
        result = jnp.einsum('hqk,khd->qhd', probs.astype(jnp.float32), value_all)
        return result.astype(jnp.bfloat16).reshape(block, D)
    blocks = lax.map(one_block, jnp.arange(LEN // block, dtype=jnp.int32))
    return blocks.reshape(LEN, D)

def reference(hidden_in, lengths, project_weight, output_weight, first_gain, first_shift, up_weight, down_weight, second_gain, second_shift, queries, positive):

    def encode(item):
        tokens, length = item
        projected = jnp.dot(tokens, project_weight, preferred_element_type=jnp.float32).astype(jnp.bfloat16)
        attended = attend(projected, length)
        mixed = jnp.dot(attended, output_weight, preferred_element_type=jnp.float32) + tokens.astype(jnp.float32)
        normed = layer_norm(mixed, first_gain, first_shift).astype(jnp.bfloat16)
        inner = jax.nn.gelu(jnp.dot(normed, up_weight, preferred_element_type=jnp.float32), approximate=False).astype(jnp.bfloat16)
        outer = lax.dot_general(inner, down_weight, (((1,), (1,)), ((), ())), preferred_element_type=jnp.float32)
        final = layer_norm(outer + normed.astype(jnp.float32), second_gain, second_shift)
        valid = (jnp.arange(LEN, dtype=jnp.int32) < length).astype(jnp.float32)
        pooled = lax.optimization_barrier(jnp.sum(final * valid[:, None], axis=0)) / length.astype(jnp.float32)
        return (final.astype(jnp.bfloat16), pooled)
    hidden_out, pooled = lax.map(encode, (hidden_in, lengths))
    embeddings = pooled / jnp.sqrt(lax.optimization_barrier(jnp.sum(pooled * pooled, axis=-1, keepdims=True)) + 1e-06)
    short_queries = (queries / jnp.sqrt(lax.optimization_barrier(jnp.sum(queries * queries, axis=-1, keepdims=True)) + 1e-06)).astype(jnp.bfloat16)
    short_passages = embeddings.astype(jnp.bfloat16)
    logits = 20.0 * jnp.dot(short_queries, short_passages.T, preferred_element_type=jnp.float32)
    chosen = positive[:, None] == jnp.arange(PASSAGES, dtype=jnp.int32)[None, :]
    picked = lax.optimization_barrier(jnp.sum(jnp.where(chosen, logits, 0.0), axis=1))
    query_loss = jnp.log(lax.optimization_barrier(jnp.sum(jnp.exp(logits), axis=1))) - picked
    return (hidden_out, embeddings, query_loss)
```

```python
import functools
import math

import jax
import jax.numpy as jnp
from jax import lax
from jax.experimental import pallas as pl
from jax.experimental.pallas import tpu as pltpu
from jax.sharding import PartitionSpec as P

HEAD_DIM = 64
PAIR = 2 * HEAD_DIM
LOW = -1e30
TILE = 256
HALVES = 2
MESH = pl.DeviceIdType.MESH
F32 = jnp.float32
BF16 = jnp.bfloat16


def layer_norm(values, gain, shift):
    average = jnp.mean(values, axis=-1, keepdims=True)
    centred = values - average
    variance = jnp.mean(centred * centred, axis=-1, keepdims=True)
    return centred * lax.rsqrt(variance + 1e-05) * gain + shift


def span(index, size):
    return pl.ds(pl.multiple_of(index * size, size), size)


def flip(index, bit):
    step = 1 << bit
    return index + (1 - 2 * ((index // step) % 2)) * step


class Gather:
    def __init__(self, source, held, send, recv, mine, order):
        self.source, self.held, self.send_sem, self.recv_sem = source, held, send, recv
        self.mine, self.order = mine, order
        self.rows = source.shape[0]

    def origin(self, piece, base):
        for place, bit in enumerate(self.order):
            if (piece >> place) & 1:
                base = flip(base, bit)
        return base

    def copy(self, stage, piece, incoming):
        peer = flip(self.mine, self.order[stage])
        owner = self.origin(piece, peer if incoming else self.mine)
        there = self.held.at[span(owner, self.rows)]
        slot = (1 << stage) - 1 + piece
        return pltpu.make_async_remote_copy(
            src_ref=self.source if piece == 0 and not incoming else there,
            dst_ref=there,
            send_sem=self.send_sem.at[slot],
            recv_sem=self.recv_sem.at[slot],
            device_id={"grp": peer},
            device_id_type=MESH,
        )

    def begin(self, stage):
        self.copy(stage, 0, False).start()

    def pass_on(self, stage, piece):
        self.copy(stage, piece, True).wait_recv()
        for later in range(stage + 1, len(self.order)):
            self.copy(later, (1 << stage) + piece, False).start()

    def drain(self):
        for stage in range(len(self.order)):
            for piece in range(1 << stage):
                self.copy(stage, piece, False).wait_send()


def kernel(
    seq_size,
    grp_size,
    tok_hbm,
    length_ref,
    wp_hbm,
    wo_hbm,
    gain1,
    shift1,
    up_hbm,
    down_hbm,
    gain2,
    shift2,
    query_ref,
    positive_ref,
    out_hbm,
    emb_out,
    loss_out,
    hid,
    wp,
    wo,
    up,
    down,
    qm,
    kbuf,
    vt,
    acc,
    high,
    summed,
    bias,
    att,
    normed,
    inner,
    outer,
    final,
    totals,
    embeds,
    local_sem,
    below_send,
    below_recv,
    above_send,
    above_recv,
    up_send,
    up_recv,
    down_send,
    down_recv,
    tot_send,
    tot_recv,
    emb_send,
    emb_recv,
):
    rank = lax.axis_index("seq")
    group = lax.axis_index("grp")
    rows, width = tok_hbm.shape[1:]
    ff = up_hbm.shape[1]
    heads = width // HEAD_DIM
    pairs = width // PAIR
    part = rows // HALVES
    length = length_ref[0]
    bits = grp_size.bit_length() - 1

    barrier = pltpu.get_barrier_semaphore()
    for step in range(1, seq_size):
        pl.semaphore_signal(
            barrier,
            inc=1,
            device_id={"seq": (rank + step) % seq_size},
            device_id_type=MESH,
        )
    for step in range(1, grp_size):
        pl.semaphore_signal(
            barrier,
            inc=1,
            device_id={"grp": (group + step) % grp_size},
            device_id_type=MESH,
        )
    loads = [
        pltpu.make_async_copy(tok_hbm.at[0], hid.at[span(rank, rows)], local_sem.at[0]),
        pltpu.make_async_copy(wp_hbm, wp, local_sem.at[1]),
        pltpu.make_async_copy(wo_hbm, wo, local_sem.at[2]),
        pltpu.make_async_copy(up_hbm, up.at[span(group, up_hbm.shape[0])], local_sem.at[3]),
        pltpu.make_async_copy(down_hbm, down.at[span(group, down_hbm.shape[0])], local_sem.at[4]),
    ]
    for load in loads:
        load.start()
    pl.semaphore_wait(barrier, seq_size - 1 + grp_size - 1)

    def chain(upward, step, half, incoming, first=False):
        way = 1 if upward else -1
        owner = rank - way * step if incoming else rank - way * (step - 1)
        there = hid.at[span(owner * HALVES + half, part)]
        slot = (step - 1) * HALVES + half
        sends, recvs = (below_send, below_recv) if upward else (above_send, above_recv)
        return pltpu.make_async_remote_copy(
            src_ref=tok_hbm.at[0, pl.ds(half * part, part)] if first else there,
            dst_ref=there,
            send_sem=sends.at[slot],
            recv_sem=recvs.at[slot],
            device_id={"seq": rank + way},
            device_id_type=MESH,
        )

    def has_next(upward):
        return rank + 1 < seq_size if upward else rank >= 1

    def holds(upward, step):
        return rank - step >= 0 if upward else rank + step < seq_size

    for half in range(HALVES):
        for upward in (True, False):

            @pl.when(has_next(upward))
            def _(upward=upward, half=half):
                chain(upward, 1, half, False, True).start()

    order = list(range(1, bits)) + [0]
    back = list(reversed(range(1, bits))) + [0]
    ups = Gather(up_hbm, up, up_send, up_recv, group, order)
    downs = Gather(down_hbm, down, down_send, down_recv, group, back)
    for stage in range(bits):
        ups.begin(stage)
        downs.begin(stage)
    events = [(stage, piece) for stage in range(bits - 1) for piece in range(1 << stage)]

    loads[0].wait()
    loads[1].wait()

    lane = lax.broadcasted_iota(jnp.int32, (1, PAIR), 1)
    left = jnp.where(lane < HEAD_DIM, 1.0, 0.0).astype(BF16)
    right = jnp.where(lane < HEAD_DIM, 0.0, 1.0).astype(BF16)
    factor = math.log2(math.e) / math.sqrt(HEAD_DIM)
    own = span(rank, rows)

    @pl.loop(0, width // TILE)
    def _(tile):
        query = jnp.dot(hid[own, :], wp[:, span(tile, TILE)], preferred_element_type=F32) * factor
        query = query.astype(BF16)
        for pair in range(TILE // PAIR):
            both = query[:, pair * PAIR : (pair + 1) * PAIR]
            at = tile * (TILE // HEAD_DIM) + 2 * pair
            qm[at] = both * left
            qm[at + 1] = both * right

    acc[...] = jnp.zeros_like(acc)
    summed[...] = jnp.zeros_like(summed)
    high[...] = jnp.full_like(high, 2 * LOW)
    ones = jnp.ones((16, rows), BF16)

    def attend(owner):
        block = span(owner, rows)

        @pl.loop(0, width // TILE)
        def _(tile):
            key = jnp.dot(
                hid[block, :],
                wp[:, pl.ds(pl.multiple_of(width + tile * TILE, TILE), TILE)],
                preferred_element_type=F32,
            )
            kbuf[:, span(tile, TILE)] = key.astype(BF16)
            value = jnp.dot(
                hid[block, :],
                wp[:, pl.ds(pl.multiple_of(2 * width + tile * TILE, TILE), TILE)],
                preferred_element_type=F32,
            )
            vt[span(tile, TILE), :] = value.T.astype(BF16)

        position = lax.broadcasted_iota(jnp.int32, (rows, PAIR), 0) + owner * rows
        bias[...] = jnp.where(position < length, 0.0, LOW)

        @pl.loop(0, pairs)
        def _(pair):
            key = kbuf[:, span(pair, PAIR)]
            for side in range(2):
                head = 2 * pair + side
                scores = lax.dot_general(
                    key, qm[head], (((1,), (1,)), ((), ())), preferred_element_type=F32
                )
                scores = scores + jnp.concatenate([bias[...]] * (rows // PAIR), axis=1)
                old = high[head, 0:1, :]
                top = jnp.maximum(old, jnp.max(scores, axis=0, keepdims=True))
                expo = jnp.exp2(scores - top).astype(BF16)
                alpha = jnp.exp2(old - top)
                value = jnp.concatenate([vt[span(head, HEAD_DIM), :], ones], axis=0)
                got = jnp.dot(value, expo, preferred_element_type=F32)
                mine = span(head, HEAD_DIM)
                acc[mine, :] = acc[mine, :] * alpha + got[:HEAD_DIM]
                summed[head] = summed[head] * alpha + got[HEAD_DIM : HEAD_DIM + 8]
                high[head] = jnp.broadcast_to(top, (8, rows))

    @pl.loop(0, 2 * seq_size - 1)
    def _(slot):
        step = (slot + 1) // 2
        upper = (slot + 1) % 2
        owner = rank - step + 2 * step * upper

        @pl.when(jnp.logical_and(upper == 0, step >= 1))
        def _():
            for half in range(HALVES):
                for upward in (True, False):

                    @pl.when(holds(upward, step))
                    def _(upward=upward, half=half):
                        chain(upward, step, half, True).wait_recv()

                        @pl.when(has_next(upward))
                        def _():
                            chain(upward, step + 1, half, False).start()

            for index, (stage, piece) in enumerate(events):

                @pl.when(step == min(1 + index, seq_size - 1))
                def _(stage=stage, piece=piece):
                    ups.pass_on(stage, piece)
                    downs.pass_on(stage, piece)

        @pl.when(jnp.logical_and(owner >= 0, owner < seq_size))
        def _():
            attend(owner)

    @pl.loop(0, pairs)
    def _(pair):
        total = acc[span(pair, PAIR), :]
        low_part = total[:HEAD_DIM] / summed[2 * pair, 0:1, :]
        high_part = total[HEAD_DIM:] / summed[2 * pair + 1, 0:1, :]
        att[:, span(pair, PAIR)] = jnp.concatenate([low_part, high_part], axis=0).T.astype(BF16)

    loads[2].wait()

    @pl.loop(0, width // TILE)
    def _(tile):
        here = span(tile, TILE)
        mixed = jnp.dot(att[...], wo[:, here], preferred_element_type=F32)
        outer[:, here] = mixed + hid[own, here].astype(F32)

    few = 64

    @pl.loop(0, rows // few)
    def _(index):
        here = span(index, few)
        normed[here, :] = layer_norm(outer[here, :], gain1[...], shift1[...]).astype(BF16)

    loads[3].wait()
    for piece in range(1 << (bits - 1)):
        ups.pass_on(bits - 1, piece)

    @pl.loop(0, ff // TILE)
    def _(tile):
        here = span(tile, TILE)
        before = jnp.dot(normed[...], up[:, here], preferred_element_type=F32)
        half = 0.5 * before
        inner[:, here] = (half + half * lax.erf(before * math.sqrt(0.5))).astype(BF16)

    loads[4].wait()
    for piece in range(1 << (bits - 1)):
        downs.pass_on(bits - 1, piece)

    @pl.loop(0, width // TILE)
    def _(tile):
        here = span(tile, TILE)
        back_again = lax.dot_general(
            inner[...], down[here, :], (((1,), (1,)), ((), ())), preferred_element_type=F32
        )
        outer[:, here] = back_again + normed[:, here].astype(F32)

    def finish(index, carry):
        here = span(index, few)
        done = layer_norm(outer[here, :], gain2[...], shift2[...])
        final[here, :] = done.astype(BF16)
        position = lax.broadcasted_iota(jnp.int32, (few, 1), 0) + (rank * rows + index * few)
        done = jnp.where(position < length, done, 0.0)
        return carry + jnp.sum(done, axis=0, keepdims=True)

    local_total = lax.fori_loop(0, rows // few, finish, jnp.zeros((1, width), F32))
    write = pltpu.make_async_copy(final, out_hbm.at[0], local_sem.at[0])
    write.start()

    totals[rank] = local_total

    def spread(ref, axis, mine, size, step, sends, recvs, incoming):
        slot = (mine - step + size) % size if incoming else mine
        return pltpu.make_async_remote_copy(
            src_ref=ref.at[slot],
            dst_ref=ref.at[slot],
            send_sem=sends.at[step - 1],
            recv_sem=recvs.at[step - 1],
            device_id={axis: (mine + step) % size},
            device_id_type=MESH,
        )

    for step in range(1, seq_size):
        spread(totals, "seq", rank, seq_size, step, tot_send, tot_recv, False).start()

    asked = query_ref[...]
    asked = asked / jnp.sqrt(jnp.sum(asked * asked, axis=-1, keepdims=True) + 1e-06)
    asked = asked.astype(BF16).astype(F32)

    for step in range(1, seq_size):
        spread(totals, "seq", rank, seq_size, step, tot_send, tot_recv, True).wait_recv()
    pooled = totals[0]
    for place in range(1, seq_size):
        pooled = pooled + totals[place]
    pooled = pooled / length.astype(F32)
    embedding = pooled / jnp.sqrt(jnp.sum(pooled * pooled, axis=-1, keepdims=True) + 1e-06)
    emb_out[...] = embedding
    embeds[group] = embedding
    for step in range(1, grp_size):
        spread(embeds, "grp", group, grp_size, step, emb_send, emb_recv, False).start()

    for step in range(1, seq_size):
        spread(totals, "seq", rank, seq_size, step, tot_send, tot_recv, False).wait_send()
        for half in range(HALVES):
            for upward in (True, False):

                @pl.when(jnp.logical_and(has_next(upward), holds(upward, step - 1)))
                def _(upward=upward, half=half, step=step):
                    chain(upward, step, half, False, step == 1).wait_send()

    ups.drain()
    downs.drain()

    for step in range(1, grp_size):
        spread(embeds, "grp", group, grp_size, step, emb_send, emb_recv, True).wait_recv()
    count = asked.shape[0]
    row = lax.broadcasted_iota(jnp.int32, (count, 1), 0)
    wanted = jnp.zeros((count, 1), jnp.int32)
    for place in range(count):
        wanted = jnp.where(row == place, positive_ref[place], wanted)
    picked = jnp.zeros((count, 1), F32)
    weight = jnp.zeros((count, 1), F32)
    for place in range(grp_size):
        short = embeds[place].astype(BF16).astype(F32)
        logit = 20.0 * jnp.sum(asked * short, axis=-1, keepdims=True)
        picked = picked + jnp.where(wanted == place, logit, 0.0)
        weight = weight + jnp.exp(logit)
    loss_out[...] = jnp.log(weight) - picked
    for step in range(1, grp_size):
        spread(embeds, "grp", group, grp_size, step, emb_send, emb_recv, False).wait_send()
    write.wait()


def body(
    seq_size,
    grp_size,
    hidden_in,
    lengths,
    project_weight,
    output_weight,
    first_gain,
    first_shift,
    up_weight,
    down_weight,
    second_gain,
    second_shift,
    queries,
    positive,
):
    rows, width = hidden_in.shape[1:]
    ff = up_weight.shape[1]
    heads = width // HEAD_DIM
    count = queries.shape[0]
    wide = lambda vector: vector.reshape(1, -1)
    vmem = pl.BlockSpec(memory_space=pltpu.VMEM)
    smem = pl.BlockSpec(memory_space=pltpu.SMEM)
    hbm = pl.BlockSpec(memory_space=pl.ANY)
    dma = pltpu.SemaphoreType.DMA
    chain_sems = [dma(((seq_size - 1) * HALVES,))] * 4
    pieces = [dma((grp_size - 1,))] * 4
    hidden_out, embedding, loss = pl.pallas_call(
        functools.partial(kernel, seq_size, grp_size),
        out_shape=[
            jax.ShapeDtypeStruct(hidden_in.shape, BF16),
            jax.ShapeDtypeStruct((1, width), F32),
            jax.ShapeDtypeStruct((count, 1), F32),
        ],
        in_specs=[hbm, smem, hbm, hbm, vmem, vmem, hbm, hbm, vmem, vmem, vmem, smem],
        out_specs=[hbm, vmem, vmem],
        scratch_shapes=[
            pltpu.VMEM((seq_size * rows, width), BF16),
            pltpu.VMEM((width, 3 * width), BF16),
            pltpu.VMEM((width, width), BF16),
            pltpu.VMEM((width, ff), BF16),
            pltpu.VMEM((width, ff), BF16),
            pltpu.VMEM((heads, rows, PAIR), BF16),
            pltpu.VMEM((rows, width), BF16),
            pltpu.VMEM((width, rows), BF16),
            pltpu.VMEM((width, rows), F32),
            pltpu.VMEM((heads, 8, rows), F32),
            pltpu.VMEM((heads, 8, rows), F32),
            pltpu.VMEM((rows, PAIR), F32),
            pltpu.VMEM((rows, width), BF16),
            pltpu.VMEM((rows, width), BF16),
            pltpu.VMEM((rows, ff), BF16),
            pltpu.VMEM((rows, width), F32),
            pltpu.VMEM((rows, width), BF16),
            pltpu.VMEM((seq_size, 1, width), F32),
            pltpu.VMEM((grp_size, 1, width), F32),
            dma((5,)),
            *chain_sems,
            *pieces,
            dma((seq_size - 1,)),
            dma((seq_size - 1,)),
            dma((grp_size - 1,)),
            dma((grp_size - 1,)),
        ],
        compiler_params=pltpu.CompilerParams(
            collective_id=0, has_side_effects=True, vmem_limit_bytes=67_043_328
        ),
        cost_estimate=pl.CostEstimate(
            flops=8 * rows * width * ff, bytes_accessed=16 * width * ff, transcendentals=rows * ff
        ),
    )(
        hidden_in,
        lengths,
        project_weight,
        output_weight,
        wide(first_gain),
        wide(first_shift),
        up_weight,
        down_weight,
        wide(second_gain),
        wide(second_shift),
        queries,
        positive,
    )
    return hidden_out, embedding, loss.reshape(count)


def solution(mesh):
    in_specs = (
        P("grp", "seq", None),
        P("grp"),
        P(),
        P(),
        P(),
        P(),
        P("grp", None),
        P("grp", None),
        P(),
        P(),
        P("grp", None),
        P("grp"),
    )
    out_specs = (P("grp", "seq", None), P("grp", None), P("grp"))
    sized = functools.partial(body, mesh.shape["seq"], mesh.shape["grp"])
    return jax.shard_map(sized, mesh=mesh, in_specs=in_specs, out_specs=out_specs, check_vma=False)
```

```python
import functools
import math

import jax
import jax.numpy as jnp
from jax import lax
from jax.experimental import pallas as pl
from jax.experimental.pallas import tpu as pltpu
from jax.sharding import PartitionSpec as P

HEAD_DIM = 64
PAIR = 2 * HEAD_DIM
LOW = -1e30
TILE = 256
HALVES = 4
STRIPS = 8
MESH = pl.DeviceIdType.MESH
F32 = jnp.float32
BF16 = jnp.bfloat16


def layer_norm(values, gain, shift):
    average = jnp.mean(values, axis=-1, keepdims=True)
    centred = values - average
    variance = jnp.mean(centred * centred, axis=-1, keepdims=True)
    return centred * lax.rsqrt(variance + 1e-05) * gain + shift


def span(index, size):
    return pl.ds(pl.multiple_of(index * size, size), size)


def flip(index, bit):
    step = 1 << bit
    return index + (1 - 2 * ((index // step) % 2)) * step


class Gather:
    def __init__(self, source, held, send, recv, mine, order):
        self.source, self.held, self.send_sem, self.recv_sem = source, held, send, recv
        self.mine, self.order = mine, order
        self.rows = source.shape[0]

    def origin(self, piece, base):
        for place, bit in enumerate(self.order):
            if (piece >> place) & 1:
                base = flip(base, bit)
        return base

    def copy(self, stage, piece, incoming):
        peer = flip(self.mine, self.order[stage])
        owner = self.origin(piece, peer if incoming else self.mine)
        there = self.held.at[span(owner, self.rows)]
        slot = (1 << stage) - 1 + piece
        return pltpu.make_async_remote_copy(
            src_ref=self.source if piece == 0 and not incoming else there,
            dst_ref=there,
            send_sem=self.send_sem.at[slot],
            recv_sem=self.recv_sem.at[slot],
            device_id={"grp": peer},
            device_id_type=MESH,
        )

    def begin(self, stage):
        self.copy(stage, 0, False).start()

    def pass_on(self, stage, piece):
        self.copy(stage, piece, True).wait_recv()
        for later in range(stage + 1, len(self.order)):
            self.copy(later, (1 << stage) + piece, False).start()

    def drain(self):
        for stage in range(len(self.order)):
            for piece in range(1 << stage):
                self.copy(stage, piece, False).wait_send()


def kernel(
    seq_size,
    grp_size,
    tok_hbm,
    length_ref,
    wp_hbm,
    wo_hbm,
    gain1_hbm,
    shift1_hbm,
    up_hbm,
    down_hbm,
    gain2_hbm,
    shift2_hbm,
    query_hbm,
    positive_ref,
    out_hbm,
    emb_hbm,
    loss_hbm,
    gain1,
    shift1,
    gain2,
    shift2,
    query_ref,
    loss_out,
    hid,
    wp,
    wo,
    up,
    down,
    qm,
    kbuf,
    vt,
    acc,
    high,
    summed,
    bias,
    scores,
    att,
    normed,
    inner,
    outer,
    final,
    totals,
    embeds,
    local_sem,
    below_send,
    below_recv,
    above_send,
    above_recv,
    up_send,
    up_recv,
    down_send,
    down_recv,
    tot_send,
    tot_recv,
    emb_send,
    emb_recv,
):
    rank = lax.axis_index("seq")
    group = lax.axis_index("grp")
    rows, width = tok_hbm.shape[1:]
    ff = up_hbm.shape[1]
    heads = width // HEAD_DIM
    pairs = width // PAIR
    part = rows // HALVES
    length = length_ref[0]
    bits = grp_size.bit_length() - 1

    barrier = pltpu.get_barrier_semaphore()
    for step in range(1, seq_size):
        pl.semaphore_signal(
            barrier,
            inc=1,
            device_id={"seq": (rank + step) % seq_size},
            device_id_type=MESH,
        )
    for step in range(1, grp_size):
        pl.semaphore_signal(
            barrier,
            inc=1,
            device_id={"grp": (group + step) % grp_size},
            device_id_type=MESH,
        )
    loads = [
        pltpu.make_async_copy(tok_hbm.at[0], hid.at[span(rank, rows)], local_sem.at[0]),
        pltpu.make_async_copy(wp_hbm, wp, local_sem.at[1]),
        pltpu.make_async_copy(wo_hbm, wo, local_sem.at[2]),
        pltpu.make_async_copy(up_hbm, up.at[span(group, up_hbm.shape[0])], local_sem.at[3]),
        pltpu.make_async_copy(down_hbm, down.at[span(group, down_hbm.shape[0])], local_sem.at[4]),
        pltpu.make_async_copy(gain1_hbm, gain1, local_sem.at[5]),
        pltpu.make_async_copy(shift1_hbm, shift1, local_sem.at[6]),
        pltpu.make_async_copy(gain2_hbm, gain2, local_sem.at[7]),
        pltpu.make_async_copy(shift2_hbm, shift2, local_sem.at[8]),
        pltpu.make_async_copy(query_hbm, query_ref, local_sem.at[9]),
    ]
    for load in loads:
        load.start()
    pl.semaphore_wait(barrier, seq_size - 1 + grp_size - 1)

    def chain(upward, step, half, incoming, first=False):
        way = 1 if upward else -1
        owner = rank - way * step if incoming else rank - way * (step - 1)
        there = hid.at[span(owner * HALVES + half, part)]
        slot = (step - 1) * HALVES + half
        sends, recvs = (below_send, below_recv) if upward else (above_send, above_recv)
        return pltpu.make_async_remote_copy(
            src_ref=tok_hbm.at[0, pl.ds(half * part, part)] if first else there,
            dst_ref=there,
            send_sem=sends.at[slot],
            recv_sem=recvs.at[slot],
            device_id={"seq": rank + way},
            device_id_type=MESH,
        )

    def has_next(upward):
        return rank + 1 < seq_size if upward else rank >= 1

    def holds(upward, step):
        return rank - step >= 0 if upward else rank + step < seq_size

    for half in range(HALVES):
        for upward in (True, False):

            @pl.when(has_next(upward))
            def _(upward=upward, half=half):
                chain(upward, 1, half, False, True).start()

    order = list(range(1, bits)) + [0]
    back = list(reversed(range(1, bits))) + [0]
    ups = Gather(up_hbm, up, up_send, up_recv, group, order)
    downs = Gather(down_hbm, down, down_send, down_recv, group, back)
    for stage in range(bits):
        ups.begin(stage)
        downs.begin(stage)
    events = [(stage, piece) for stage in range(bits - 1) for piece in range(1 << stage)]
    early, late = events[: seq_size - 2], events[seq_size - 2 :]

    loads[0].wait()
    loads[1].wait()

    factor = math.log2(math.e) / math.sqrt(HEAD_DIM)
    own = span(rank, rows)

    @pl.loop(0, width // TILE, unroll=2)
    def _(tile):
        query = jnp.dot(hid[own, :], wp[:, span(tile, TILE)], preferred_element_type=F32) * factor
        query = query.T.astype(BF16)
        for pair in range(TILE // PAIR):
            at = tile * (TILE // HEAD_DIM) + 2 * pair
            here = pair * PAIR
            blank = jnp.zeros((HEAD_DIM, rows), BF16)
            qm[at] = jnp.concatenate([query[here : here + HEAD_DIM], blank], axis=0)
            qm[at + 1] = jnp.concatenate([blank, query[here + HEAD_DIM : here + PAIR]], axis=0)

    acc[...] = jnp.zeros_like(acc)
    summed[...] = jnp.zeros_like(summed)
    high[...] = jnp.full_like(high, 2 * LOW)
    ones = jnp.ones((16, part), BF16)

    def attend(unit):
        block = span(unit, part)

        @pl.loop(0, width // TILE, unroll=2)
        def _(tile):
            key = jnp.dot(
                hid[block, :],
                wp[:, pl.ds(pl.multiple_of(width + tile * TILE, TILE), TILE)],
                preferred_element_type=F32,
            )
            kbuf[:, span(tile, TILE)] = key.astype(BF16)
            value = jnp.dot(
                hid[block, :],
                wp[:, pl.ds(pl.multiple_of(2 * width + tile * TILE, TILE), TILE)],
                preferred_element_type=F32,
            )
            vt[span(tile, TILE), :] = value.T.astype(BF16)

        position = lax.broadcasted_iota(jnp.int32, (part, PAIR), 0) + unit * part
        bias[...] = jnp.where(position < length, 0.0, LOW)

        def score(pair, place):
            key = kbuf[:, pl.ds(pair * PAIR, PAIR)]
            shift = jnp.concatenate([bias[...]] * (rows // PAIR), axis=1)
            for side in range(2):
                scores[place, side] = shift + jnp.dot(
                    key, qm[2 * pair + side], preferred_element_type=F32
                )

        def weigh(pair, place):
            for side in range(2):
                head = 2 * pair + side
                score_now = scores[place, side]
                old = high[head, 0:1, :]
                top = jnp.maximum(old, jnp.max(score_now, axis=0, keepdims=True))
                expo = jnp.exp2(score_now - top).astype(BF16)
                alpha = jnp.exp2(old - top)
                value = jnp.concatenate([vt[pl.ds(head * HEAD_DIM, HEAD_DIM), :], ones], axis=0)
                got = jnp.dot(value, expo, preferred_element_type=F32)
                mine = pl.ds(head * HEAD_DIM, HEAD_DIM)
                acc[mine, :] = acc[mine, :] * alpha + got[:HEAD_DIM]
                summed[head] = summed[head] * alpha + got[HEAD_DIM : HEAD_DIM + 8]
                high[head] = jnp.broadcast_to(top, (8, rows))

        score(0, 0)
        for pair in range(pairs):
            if pair + 1 < pairs:
                score(pair + 1, (pair + 1) % 2)
            weigh(pair, pair % 2)

    @pl.loop(0, seq_size * HALVES)
    def _(slot):
        step = slot // HALVES
        half = slot % HALVES
        for upward in (True, False):

            @pl.when(jnp.logical_and(step >= 1, holds(upward, step)))
            def _(upward=upward):
                chain(upward, step, half, True).wait_recv()

                @pl.when(has_next(upward))
                def _():
                    chain(upward, step + 1, half, False).start()

        for index, (stage, piece) in enumerate(early):

            @pl.when(slot == (2 + index) * HALVES - 1)
            def _(stage=stage, piece=piece):
                ups.pass_on(stage, piece)
                downs.pass_on(stage, piece)

        @pl.loop(0, 2)
        def _(upper):
            owner = rank - step + 2 * step * upper

            @pl.when((owner >= 0) & (owner < seq_size) & (step + upper >= 1))
            def _():
                attend(owner * HALVES + half)

    for stage, piece in late:
        ups.pass_on(stage, piece)
        downs.pass_on(stage, piece)

    @pl.loop(0, pairs, unroll=4)
    def _(pair):
        total = acc[span(pair, PAIR), :]
        low_part = total[:HEAD_DIM] * (1.0 / summed[2 * pair, 0:1, :])
        high_part = total[HEAD_DIM:] * (1.0 / summed[2 * pair + 1, 0:1, :])
        att[:, span(pair, PAIR)] = jnp.concatenate([low_part, high_part], axis=0).T.astype(BF16)

    loads[2].wait()

    @pl.loop(0, width // TILE, unroll=2)
    def _(tile):
        here = span(tile, TILE)
        mixed = jnp.dot(att[...], wo[:, here], preferred_element_type=F32)
        outer[:, here] = mixed + hid[own, here].astype(F32)

    for load in loads[5:]:
        load.wait()
    few = 128

    @pl.loop(0, rows // few, unroll=2)
    def _(index):
        here = span(index, few)
        normed[here, :] = layer_norm(outer[here, :], gain1[...], shift1[...]).astype(BF16)

    loads[3].wait()
    for piece in range(1 << (bits - 1)):
        ups.pass_on(bits - 1, piece)

    @pl.loop(0, ff // TILE, unroll=4)
    def _(tile):
        here = span(tile, TILE)
        before = jnp.dot(normed[...], up[:, here], preferred_element_type=F32)
        half = 0.5 * before
        inner[:, here] = (half + half * lax.erf(before * math.sqrt(0.5))).astype(BF16)

    loads[4].wait()
    for piece in range(1 << (bits - 1)):
        downs.pass_on(bits - 1, piece)

    @pl.loop(0, width // TILE, unroll=2)
    def _(tile):
        here = span(tile, TILE)
        back_again = lax.dot_general(
            inner[...], down[here, :], (((1,), (1,)), ((), ())), preferred_element_type=F32
        )
        outer[:, here] = back_again + normed[:, here].astype(F32)

    def finish(index, carry):
        here = span(index, few)
        done = layer_norm(outer[here, :], gain2[...], shift2[...])
        final[here, :] = done.astype(BF16)
        position = lax.broadcasted_iota(jnp.int32, (few, 1), 0) + (rank * rows + index * few)
        done = jnp.where(position < length, done, 0.0)
        return carry + jnp.sum(done, axis=0, keepdims=True)

    local_total = lax.fori_loop(
        0, rows // few, finish, jnp.zeros((1, width), F32), unroll=2
    )
    write = pltpu.make_async_copy(final, out_hbm.at[0], local_sem.at[0])
    write.start()

    totals[rank] = local_total

    def spread(ref, axis, mine, size, step, sends, recvs, incoming):
        slot = (mine - step + size) % size if incoming else mine
        return pltpu.make_async_remote_copy(
            src_ref=ref.at[slot],
            dst_ref=ref.at[slot],
            send_sem=sends.at[step - 1],
            recv_sem=recvs.at[step - 1],
            device_id={axis: (mine + step) % size},
            device_id_type=MESH,
        )

    for step in range(1, seq_size):
        spread(totals, "seq", rank, seq_size, step, tot_send, tot_recv, False).start()

    asked = query_ref[...]
    asked = asked / jnp.sqrt(jnp.sum(asked * asked, axis=-1, keepdims=True) + 1e-06)
    asked = asked.astype(BF16).astype(F32)

    for step in range(1, seq_size):
        spread(totals, "seq", rank, seq_size, step, tot_send, tot_recv, True).wait_recv()
    pooled = totals[0]
    for place in range(1, seq_size):
        pooled = pooled + totals[place]
    pooled = pooled / length.astype(F32)
    embedding = pooled / jnp.sqrt(jnp.sum(pooled * pooled, axis=-1, keepdims=True) + 1e-06)
    embeds[group] = embedding
    keep = pltpu.make_async_copy(embeds.at[group], emb_hbm, local_sem.at[1])
    keep.start()
    for step in range(1, grp_size):
        spread(embeds, "grp", group, grp_size, step, emb_send, emb_recv, False).start()

    for step in range(1, seq_size):
        spread(totals, "seq", rank, seq_size, step, tot_send, tot_recv, False).wait_send()
        for half in range(HALVES):
            for upward in (True, False):

                @pl.when(jnp.logical_and(has_next(upward), holds(upward, step - 1)))
                def _(upward=upward, half=half, step=step):
                    chain(upward, step, half, False, step == 1).wait_send()

    ups.drain()
    downs.drain()

    for step in range(1, grp_size):
        spread(embeds, "grp", group, grp_size, step, emb_send, emb_recv, True).wait_recv()
    count = asked.shape[0]
    row = lax.broadcasted_iota(jnp.int32, (count, 1), 0)
    wanted = jnp.zeros((count, 1), jnp.int32)
    for place in range(count):
        wanted = jnp.where(row == place, positive_ref[place], wanted)
    picked = jnp.zeros((count, 1), F32)
    weight = jnp.zeros((count, 1), F32)
    for place in range(grp_size):
        short = embeds[place].astype(BF16).astype(F32)
        logit = 20.0 * jnp.sum(asked * short, axis=-1, keepdims=True)
        picked = picked + jnp.where(wanted == place, logit, 0.0)
        weight = weight + jnp.exp(logit)
    loss = jnp.log(weight) - picked
    loss_out[...] = jnp.broadcast_to(loss, (count, PAIR)).T[0:1, :]
    give = pltpu.make_async_copy(loss_out, loss_hbm, local_sem.at[2])
    give.start()
    for step in range(1, grp_size):
        spread(embeds, "grp", group, grp_size, step, emb_send, emb_recv, False).wait_send()
    write.wait()
    keep.wait()
    give.wait()


def hand_over(hidden, embedding, loss, hidden_out, embedding_out, loss_out, *held):
    strips, small, short, come, go = held
    strip = strips.shape[0] // STRIPS
    at = lambda index: pl.ds(index * strip, strip)
    legs = [(hidden.at[0, at(i)], strips.at[at(i)], hidden_out.at[0, at(i)]) for i in range(STRIPS)]
    legs += [(embedding, small, embedding_out), (loss, short, loss_out)]
    comes = [pltpu.make_async_copy(leg[0], leg[1], come.at[i]) for i, leg in enumerate(legs)]
    goes = [pltpu.make_async_copy(leg[1], leg[2], go.at[i]) for i, leg in enumerate(legs)]
    for copy in comes:
        copy.start()
    for index in range(len(legs)):
        comes[index].wait()
        goes[index].start()
    for copy in goes:
        copy.wait()


def body(
    seq_size,
    grp_size,
    hidden_in,
    lengths,
    project_weight,
    output_weight,
    first_gain,
    first_shift,
    up_weight,
    down_weight,
    second_gain,
    second_shift,
    queries,
    positive,
):
    rows, width = hidden_in.shape[1:]
    ff = up_weight.shape[1]
    heads = width // HEAD_DIM
    count = queries.shape[0]
    wide = lambda vector: vector.reshape(1, -1)
    smem = pl.BlockSpec(memory_space=pltpu.SMEM)
    hbm = pl.BlockSpec(memory_space=pl.ANY)
    dma = pltpu.SemaphoreType.DMA
    chain_sems = [dma(((seq_size - 1) * HALVES,))] * 4
    pieces = [dma((grp_size - 1,))] * 4
    hidden_out, embedding, loss = pl.pallas_call(
        functools.partial(kernel, seq_size, grp_size),
        out_shape=[
            jax.ShapeDtypeStruct(hidden_in.shape, BF16),
            jax.ShapeDtypeStruct((1, width), F32),
            jax.ShapeDtypeStruct((1, count), F32),
        ],
        in_specs=[hbm, smem, hbm, hbm, hbm, hbm, hbm, hbm, hbm, hbm, hbm, smem],
        out_specs=[hbm, hbm, hbm],
        scratch_shapes=[
            *[pltpu.VMEM((1, width), F32)] * 4,
            pltpu.VMEM((count, width), F32),
            pltpu.VMEM((1, count), F32),
            pltpu.VMEM((seq_size * rows, width), BF16),
            pltpu.VMEM((width, 3 * width), BF16),
            pltpu.VMEM((width, width), BF16),
            pltpu.VMEM((width, ff), BF16),
            pltpu.VMEM((width, ff), BF16),
            pltpu.VMEM((heads, PAIR, rows), BF16),
            pltpu.VMEM((rows // HALVES, width), BF16),
            pltpu.VMEM((width, rows // HALVES), BF16),
            pltpu.VMEM((width, rows), F32),
            pltpu.VMEM((heads, 8, rows), F32),
            pltpu.VMEM((heads, 8, rows), F32),
            pltpu.VMEM((rows // HALVES, PAIR), F32),
            pltpu.VMEM((2, 2, rows // HALVES, rows), F32),
            pltpu.VMEM((rows, width), BF16),
            pltpu.VMEM((rows, width), BF16),
            pltpu.VMEM((rows, ff), BF16),
            pltpu.VMEM((rows, width), F32),
            pltpu.VMEM((rows, width), BF16),
            pltpu.VMEM((seq_size, 1, width), F32),
            pltpu.VMEM((grp_size, 1, width), F32),
            dma((10,)),
            *chain_sems,
            *pieces,
            dma((seq_size - 1,)),
            dma((seq_size - 1,)),
            dma((grp_size - 1,)),
            dma((grp_size - 1,)),
        ],
        compiler_params=pltpu.CompilerParams(
            collective_id=0, has_side_effects=True, vmem_limit_bytes=54 << 20
        ),
        cost_estimate=pl.CostEstimate(
            flops=8 * rows * width * ff, bytes_accessed=16 * width * ff, transcendentals=rows * ff
        ),
    )(
        hidden_in,
        lengths,
        project_weight,
        output_weight,
        wide(first_gain),
        wide(first_shift),
        up_weight,
        down_weight,
        wide(second_gain),
        wide(second_shift),
        queries,
        positive,
    )
    hidden_out, embedding, loss = pl.pallas_call(
        hand_over,
        out_shape=[
            jax.ShapeDtypeStruct(hidden_out.shape, BF16),
            jax.ShapeDtypeStruct(embedding.shape, F32),
            jax.ShapeDtypeStruct(loss.shape, F32),
        ],
        in_specs=[hbm, hbm, hbm],
        out_specs=[hbm, hbm, hbm],
        scratch_shapes=[
            pltpu.VMEM((rows, width), BF16),
            pltpu.VMEM(embedding.shape, F32),
            pltpu.VMEM(loss.shape, F32),
            dma((STRIPS + 2,)),
            dma((STRIPS + 2,)),
        ],
        cost_estimate=pl.CostEstimate(
            flops=rows * width, bytes_accessed=4 * rows * width, transcendentals=0
        ),
    )(hidden_out, embedding, loss)
    return hidden_out, embedding, loss.reshape(count)


def solution(mesh):
    in_specs = (
        P("grp", "seq", None),
        P("grp"),
        P(),
        P(),
        P(),
        P(),
        P("grp", None),
        P("grp", None),
        P(),
        P(),
        P("grp", None),
        P("grp"),
    )
    out_specs = (P("grp", "seq", None), P("grp", None), P("grp"))
    sized = functools.partial(body, mesh.shape["seq"], mesh.shape["grp"])
    return jax.shard_map(sized, mesh=mesh, in_specs=in_specs, out_specs=out_specs, check_vma=False)
```

```python
import functools
import math

import jax
import jax.numpy as jnp
from jax import lax
from jax.experimental import pallas as pl
from jax.experimental.pallas import tpu as pltpu
from jax.sharding import PartitionSpec as P

HEAD_DIM = 64
PAIR = 2 * HEAD_DIM
LOW = -1e30
TILE = 256
WIDE = 512
HALVES = 4
STRIPS = 8
MESH = pl.DeviceIdType.MESH
F32 = jnp.float32
BF16 = jnp.bfloat16


def layer_norm(values, gain, shift):
    average = jnp.mean(values, axis=-1, keepdims=True)
    centred = values - average
    variance = jnp.mean(centred * centred, axis=-1, keepdims=True)
    return centred * lax.rsqrt(variance + 1e-05) * gain + shift


def span(index, size):
    return pl.ds(pl.multiple_of(index * size, size), size)


def flip(index, bit):
    step = 1 << bit
    return index + (1 - 2 * ((index // step) % 2)) * step


class Gather:
    def __init__(self, source, held, send, recv, mine, order):
        self.source, self.held, self.send_sem, self.recv_sem = source, held, send, recv
        self.mine, self.order = mine, order
        self.rows = source.shape[0]

    def origin(self, piece, base):
        for place, bit in enumerate(self.order):
            if (piece >> place) & 1:
                base = flip(base, bit)
        return base

    def copy(self, stage, piece, incoming):
        peer = flip(self.mine, self.order[stage])
        owner = self.origin(piece, peer if incoming else self.mine)
        there = self.held.at[span(owner, self.rows)]
        slot = (1 << stage) - 1 + piece
        return pltpu.make_async_remote_copy(
            src_ref=self.source if piece == 0 and not incoming else there,
            dst_ref=there,
            send_sem=self.send_sem.at[slot],
            recv_sem=self.recv_sem.at[slot],
            device_id={"grp": peer},
            device_id_type=MESH,
        )

    def begin(self, stage):
        self.copy(stage, 0, False).start()

    def pass_on(self, stage, piece):
        self.copy(stage, piece, True).wait_recv()
        for later in range(stage + 1, len(self.order)):
            self.copy(later, (1 << stage) + piece, False).start()

    def drain(self):
        for stage in range(len(self.order)):
            for piece in range(1 << stage):
                self.copy(stage, piece, False).wait_send()


def kernel(
    seq_size,
    grp_size,
    tok_hbm,
    length_ref,
    wp_hbm,
    wo_hbm,
    gain1_hbm,
    shift1_hbm,
    up_hbm,
    down_hbm,
    gain2_hbm,
    shift2_hbm,
    out_hbm,
    table_hbm,
    gain1,
    shift1,
    gain2,
    shift2,
    hid,
    wp,
    wo,
    up,
    down,
    qm,
    kbuf,
    vt,
    acc,
    high,
    summed,
    bias,
    scores,
    att,
    normed,
    inner,
    outer,
    final,
    totals,
    embeds,
    local_sem,
    below_send,
    below_recv,
    above_send,
    above_recv,
    up_send,
    up_recv,
    down_send,
    down_recv,
    tot_send,
    tot_recv,
    emb_send,
    emb_recv,
):
    rank = lax.axis_index("seq")
    group = lax.axis_index("grp")
    rows, width = tok_hbm.shape[1:]
    ff = up_hbm.shape[1]
    heads = width // HEAD_DIM
    pairs = width // PAIR
    part = rows // HALVES
    length = length_ref[0]
    bits = grp_size.bit_length() - 1

    barrier = pltpu.get_barrier_semaphore()
    for step in range(1, seq_size):
        pl.semaphore_signal(
            barrier,
            inc=1,
            device_id={"seq": (rank + step) % seq_size},
            device_id_type=MESH,
        )
    for step in range(1, grp_size):
        pl.semaphore_signal(
            barrier,
            inc=1,
            device_id={"grp": (group + step) % grp_size},
            device_id_type=MESH,
        )
    loads = [
        pltpu.make_async_copy(tok_hbm.at[0], hid.at[span(rank, rows)], local_sem.at[0]),
        pltpu.make_async_copy(wp_hbm, wp, local_sem.at[1]),
        pltpu.make_async_copy(wo_hbm, wo, local_sem.at[2]),
        pltpu.make_async_copy(up_hbm, up.at[span(group, up_hbm.shape[0])], local_sem.at[3]),
        pltpu.make_async_copy(down_hbm, down.at[span(group, down_hbm.shape[0])], local_sem.at[4]),
        pltpu.make_async_copy(gain1_hbm, gain1, local_sem.at[5]),
        pltpu.make_async_copy(shift1_hbm, shift1, local_sem.at[6]),
        pltpu.make_async_copy(gain2_hbm, gain2, local_sem.at[7]),
        pltpu.make_async_copy(shift2_hbm, shift2, local_sem.at[8]),
    ]
    pl.semaphore_wait(barrier, seq_size - 1 + grp_size - 1)

    def chain(upward, step, half, incoming, first=False):
        way = 1 if upward else -1
        owner = rank - way * step if incoming else rank - way * (step - 1)
        there = hid.at[span(owner * HALVES + half, part)]
        slot = (step - 1) * HALVES + half
        sends, recvs = (below_send, below_recv) if upward else (above_send, above_recv)
        return pltpu.make_async_remote_copy(
            src_ref=tok_hbm.at[0, pl.ds(half * part, part)] if first else there,
            dst_ref=there,
            send_sem=sends.at[slot],
            recv_sem=recvs.at[slot],
            device_id={"seq": rank + way},
            device_id_type=MESH,
        )

    def has_next(upward):
        return rank + 1 < seq_size if upward else rank >= 1

    def holds(upward, step):
        return rank - step >= 0 if upward else rank + step < seq_size

    for half in range(HALVES):
        for upward in (True, False):

            @pl.when(has_next(upward))
            def _(upward=upward, half=half):
                chain(upward, 1, half, False, True).start()

    for load in loads[:2]:
        load.start()
    order = list(range(1, bits)) + [0]
    back = list(reversed(range(1, bits))) + [0]
    ups = Gather(up_hbm, up, up_send, up_recv, group, order)
    downs = Gather(down_hbm, down, down_send, down_recv, group, back)
    for stage in range(bits):
        ups.begin(stage)
        downs.begin(stage)
    for load in loads[2:]:
        load.start()
    events = [(stage, piece) for stage in range(bits - 1) for piece in range(1 << stage)]
    early, late = events[: seq_size - 2], events[seq_size - 2 :]

    loads[0].wait()
    loads[1].wait()

    factor = math.log2(math.e) / math.sqrt(HEAD_DIM)
    own = span(rank, rows)

    @pl.loop(0, width // TILE, unroll=2)
    def _(tile):
        query = jnp.dot(hid[own, :], wp[:, span(tile, TILE)], preferred_element_type=F32) * factor
        query = query.T.astype(BF16)
        for pair in range(TILE // PAIR):
            at = tile * (TILE // HEAD_DIM) + 2 * pair
            here = pair * PAIR
            blank = jnp.zeros((HEAD_DIM, rows), BF16)
            qm[at] = jnp.concatenate([query[here : here + HEAD_DIM], blank], axis=0)
            qm[at + 1] = jnp.concatenate([blank, query[here + HEAD_DIM : here + PAIR]], axis=0)

    acc[...] = jnp.zeros_like(acc)
    summed[...] = jnp.zeros_like(summed)
    high[...] = jnp.full_like(high, 2 * LOW)
    ones = jnp.ones((16, part), BF16)

    def attend(unit):
        block = span(unit, part)

        @pl.loop(0, width // TILE, unroll=2)
        def _(tile):
            key = jnp.dot(
                hid[block, :],
                wp[:, pl.ds(pl.multiple_of(width + tile * TILE, TILE), TILE)],
                preferred_element_type=F32,
            )
            kbuf[:, span(tile, TILE)] = key.astype(BF16)
            value = jnp.dot(
                hid[block, :],
                wp[:, pl.ds(pl.multiple_of(2 * width + tile * TILE, TILE), TILE)],
                preferred_element_type=F32,
            )
            vt[span(tile, TILE), :] = value.T.astype(BF16)

        position = lax.broadcasted_iota(jnp.int32, (part, PAIR), 0) + unit * part
        bias[...] = jnp.where(position < length, 0.0, LOW)

        def score(pair, place):
            key = kbuf[:, pl.ds(pair * PAIR, PAIR)]
            shift = jnp.concatenate([bias[...]] * (rows // PAIR), axis=1)
            for side in range(2):
                scores[place, side] = shift + jnp.dot(
                    key, qm[2 * pair + side], preferred_element_type=F32
                )

        def weigh(pair, place):
            for side in range(2):
                head = 2 * pair + side
                score_now = scores[place, side]
                old = high[head, 0:1, :]
                top = jnp.maximum(old, jnp.max(score_now, axis=0, keepdims=True))
                expo = jnp.exp2(score_now - top).astype(BF16)
                alpha = jnp.exp2(old - top)
                value = jnp.concatenate([vt[pl.ds(head * HEAD_DIM, HEAD_DIM), :], ones], axis=0)
                got = jnp.dot(value, expo, preferred_element_type=F32)
                mine = pl.ds(head * HEAD_DIM, HEAD_DIM)
                acc[mine, :] = acc[mine, :] * alpha + got[:HEAD_DIM]
                summed[head] = summed[head] * alpha + got[HEAD_DIM : HEAD_DIM + 8]
                high[head] = jnp.broadcast_to(top, (8, rows))

        score(0, 0)
        for pair in range(pairs):
            if pair + 1 < pairs:
                score(pair + 1, (pair + 1) % 2)
            weigh(pair, pair % 2)

    @pl.loop(0, seq_size * HALVES)
    def _(slot):
        step = slot // HALVES
        half = slot % HALVES
        for upward in (True, False):

            @pl.when(jnp.logical_and(step >= 1, holds(upward, step)))
            def _(upward=upward):
                chain(upward, step, half, True).wait_recv()

                @pl.when(has_next(upward))
                def _():
                    chain(upward, step + 1, half, False).start()

        for index, (stage, piece) in enumerate(early):

            @pl.when(slot == (2 + index) * HALVES - 1)
            def _(stage=stage, piece=piece):
                ups.pass_on(stage, piece)
                downs.pass_on(stage, piece)

        @pl.loop(0, 2)
        def _(upper):
            owner = rank - step + 2 * step * upper

            @pl.when((owner >= 0) & (owner < seq_size) & (step + upper >= 1))
            def _():
                attend(owner * HALVES + half)

    for stage, piece in late:
        ups.pass_on(stage, piece)
        downs.pass_on(stage, piece)

    @pl.loop(0, pairs, unroll=4)
    def _(pair):
        total = acc[span(pair, PAIR), :]
        low_part = total[:HEAD_DIM] * (1.0 / summed[2 * pair, 0:1, :])
        high_part = total[HEAD_DIM:] * (1.0 / summed[2 * pair + 1, 0:1, :])
        att[:, span(pair, PAIR)] = jnp.concatenate([low_part, high_part], axis=0).T.astype(BF16)

    loads[2].wait()

    @pl.loop(0, width // WIDE, unroll=2)
    def _(tile):
        here = span(tile, WIDE)
        mixed = jnp.dot(att[...], wo[:, here], preferred_element_type=F32)
        outer[:, here] = mixed + hid[own, here].astype(F32)

    for load in loads[5:]:
        load.wait()
    few = 128

    @pl.loop(0, rows // few, unroll=2)
    def _(index):
        here = span(index, few)
        normed[here, :] = layer_norm(outer[here, :], gain1[...], shift1[...]).astype(BF16)

    loads[3].wait()
    for piece in range(1 << (bits - 1)):
        ups.pass_on(bits - 1, piece)

    @pl.loop(0, ff // WIDE, unroll=4)
    def _(tile):
        here = span(tile, WIDE)
        before = jnp.dot(normed[...], up[:, here], preferred_element_type=F32)
        half = 0.5 * before
        inner[:, here] = (half + half * lax.erf(before * math.sqrt(0.5))).astype(BF16)

    loads[4].wait()
    for piece in range(1 << (bits - 1)):
        downs.pass_on(bits - 1, piece)

    @pl.loop(0, width // WIDE, unroll=2)
    def _(tile):
        here = span(tile, WIDE)
        back_again = lax.dot_general(
            inner[...], down[here, :], (((1,), (1,)), ((), ())), preferred_element_type=F32
        )
        outer[:, here] = back_again + normed[:, here].astype(F32)

    def finish(index, carry):
        here = span(index, few)
        done = layer_norm(outer[here, :], gain2[...], shift2[...])
        final[here, :] = done.astype(BF16)
        position = lax.broadcasted_iota(jnp.int32, (few, 1), 0) + (rank * rows + index * few)
        done = jnp.where(position < length, done, 0.0)
        return carry + jnp.sum(done, axis=0, keepdims=True)

    local_total = lax.fori_loop(
        0, rows // few, finish, jnp.zeros((1, width), F32), unroll=2
    )
    write = pltpu.make_async_copy(final, out_hbm.at[0], local_sem.at[0])
    totals[rank] = local_total

    def spread(ref, axis, mine, size, step, sends, recvs, incoming):
        slot = (mine - step + size) % size if incoming else mine
        return pltpu.make_async_remote_copy(
            src_ref=ref.at[slot],
            dst_ref=ref.at[slot],
            send_sem=sends.at[step - 1],
            recv_sem=recvs.at[step - 1],
            device_id={axis: (mine + step) % size},
            device_id_type=MESH,
        )

    for step in range(1, seq_size):
        spread(totals, "seq", rank, seq_size, step, tot_send, tot_recv, False).start()
    write.start()

    for step in range(1, seq_size):
        spread(totals, "seq", rank, seq_size, step, tot_send, tot_recv, True).wait_recv()
    pooled = totals[0]
    for place in range(1, seq_size):
        pooled = pooled + totals[place]
    pooled = pooled / length.astype(F32)
    embedding = pooled / jnp.sqrt(jnp.sum(pooled * pooled, axis=-1, keepdims=True) + 1e-06)
    embeds[group] = embedding
    for step in range(1, grp_size):
        spread(embeds, "grp", group, grp_size, step, emb_send, emb_recv, False).start()

    for step in range(1, seq_size):
        spread(totals, "seq", rank, seq_size, step, tot_send, tot_recv, False).wait_send()
        for half in range(HALVES):
            for upward in (True, False):

                @pl.when(jnp.logical_and(has_next(upward), holds(upward, step - 1)))
                def _(upward=upward, half=half, step=step):
                    chain(upward, step, half, False, step == 1).wait_send()

    ups.drain()
    downs.drain()

    for step in range(1, grp_size):
        spread(embeds, "grp", group, grp_size, step, emb_send, emb_recv, True).wait_recv()
    keep = pltpu.make_async_copy(embeds, table_hbm, local_sem.at[1])
    keep.start()
    for step in range(1, grp_size):
        spread(embeds, "grp", group, grp_size, step, emb_send, emb_recv, False).wait_send()
    write.wait()
    keep.wait()


def hand_over(hidden, table_hbm, query_hbm, positive_ref, hidden_out, emb_out, loss_out, *held):
    strips, table, asked_ref, short, come, go = held
    strip = strips.shape[0] // STRIPS
    at = lambda index: pl.ds(index * strip, strip)
    group = lax.axis_index("grp")
    legs = [(table_hbm, table), (query_hbm, asked_ref)]
    legs += [(hidden.at[0, at(i)], strips.at[at(i)]) for i in range(STRIPS)]
    comes = [pltpu.make_async_copy(*leg, come.at[i]) for i, leg in enumerate(legs)]
    goes = [(table.at[group], emb_out), (short, loss_out)]
    goes += [(strips.at[at(i)], hidden_out.at[0, at(i)]) for i in range(STRIPS)]
    goes = [pltpu.make_async_copy(*leg, go.at[i]) for i, leg in enumerate(goes)]
    for copy in comes:
        copy.start()
    comes[0].wait()
    comes[1].wait()
    goes[0].start()
    for index in range(STRIPS):
        comes[2 + index].wait()
        goes[2 + index].start()
    asked = asked_ref[...]
    asked = asked / jnp.sqrt(jnp.sum(asked * asked, axis=-1, keepdims=True) + 1e-06)
    asked = asked.astype(BF16).astype(F32)
    count = asked.shape[0]
    row = lax.broadcasted_iota(jnp.int32, (count, 1), 0)
    wanted = jnp.zeros((count, 1), jnp.int32)
    for place in range(count):
        wanted = jnp.where(row == place, positive_ref[place], wanted)
    picked = jnp.zeros((count, 1), F32)
    weight = jnp.zeros((count, 1), F32)
    for place in range(table.shape[0]):
        passage = table[place].astype(BF16).astype(F32)
        logit = 20.0 * jnp.sum(asked * passage, axis=-1, keepdims=True)
        picked = picked + jnp.where(wanted == place, logit, 0.0)
        weight = weight + jnp.exp(logit)
    loss = jnp.log(weight) - picked
    short[...] = jnp.broadcast_to(loss, (count, PAIR)).T[0:1, :]
    goes[1].start()
    for copy in goes:
        copy.wait()


def body(
    seq_size,
    grp_size,
    hidden_in,
    lengths,
    project_weight,
    output_weight,
    first_gain,
    first_shift,
    up_weight,
    down_weight,
    second_gain,
    second_shift,
    queries,
    positive,
):
    rows, width = hidden_in.shape[1:]
    ff = up_weight.shape[1]
    heads = width // HEAD_DIM
    count = queries.shape[0]
    wide = lambda vector: vector.reshape(1, -1)
    smem = pl.BlockSpec(memory_space=pltpu.SMEM)
    hbm = pl.BlockSpec(memory_space=pl.ANY)
    dma = pltpu.SemaphoreType.DMA
    chain_sems = [dma(((seq_size - 1) * HALVES,))] * 4
    pieces = [dma((grp_size - 1,))] * 4
    hidden_out, table = pl.pallas_call(
        functools.partial(kernel, seq_size, grp_size),
        out_shape=[
            jax.ShapeDtypeStruct(hidden_in.shape, BF16),
            jax.ShapeDtypeStruct((grp_size, 1, width), F32),
        ],
        in_specs=[hbm, smem, hbm, hbm, hbm, hbm, hbm, hbm, hbm, hbm],
        out_specs=[hbm, hbm],
        scratch_shapes=[
            *[pltpu.VMEM((1, width), F32)] * 4,
            pltpu.VMEM((seq_size * rows, width), BF16),
            pltpu.VMEM((width, 3 * width), BF16),
            pltpu.VMEM((width, width), BF16),
            pltpu.VMEM((width, ff), BF16),
            pltpu.VMEM((width, ff), BF16),
            pltpu.VMEM((heads, PAIR, rows), BF16),
            pltpu.VMEM((rows // HALVES, width), BF16),
            pltpu.VMEM((width, rows // HALVES), BF16),
            pltpu.VMEM((width, rows), F32),
            pltpu.VMEM((heads, 8, rows), F32),
            pltpu.VMEM((heads, 8, rows), F32),
            pltpu.VMEM((rows // HALVES, PAIR), F32),
            pltpu.VMEM((2, 2, rows // HALVES, rows), F32),
            pltpu.VMEM((rows, width), BF16),
            pltpu.VMEM((rows, width), BF16),
            pltpu.VMEM((rows, ff), BF16),
            pltpu.VMEM((rows, width), F32),
            pltpu.VMEM((rows, width), BF16),
            pltpu.VMEM((seq_size, 1, width), F32),
            pltpu.VMEM((grp_size, 1, width), F32),
            dma((9,)),
            *chain_sems,
            *pieces,
            dma((seq_size - 1,)),
            dma((seq_size - 1,)),
            dma((grp_size - 1,)),
            dma((grp_size - 1,)),
        ],
        compiler_params=pltpu.CompilerParams(
            collective_id=0, has_side_effects=True, vmem_limit_bytes=54 << 20
        ),
        cost_estimate=pl.CostEstimate(
            flops=8 * rows * width * ff, bytes_accessed=16 * width * ff, transcendentals=rows * ff
        ),
    )(
        hidden_in,
        lengths,
        project_weight,
        output_weight,
        wide(first_gain),
        wide(first_shift),
        up_weight,
        down_weight,
        wide(second_gain),
        wide(second_shift),
    )
    hidden_out, embedding, loss = pl.pallas_call(
        hand_over,
        out_shape=[
            jax.ShapeDtypeStruct(hidden_out.shape, BF16),
            jax.ShapeDtypeStruct((1, width), F32),
            jax.ShapeDtypeStruct((1, count), F32),
        ],
        in_specs=[hbm, hbm, hbm, smem],
        out_specs=[hbm, hbm, hbm],
        scratch_shapes=[
            pltpu.VMEM((rows, width), BF16),
            pltpu.VMEM(table.shape, F32),
            pltpu.VMEM((count, width), F32),
            pltpu.VMEM((1, count), F32),
            dma((STRIPS + 2,)),
            dma((STRIPS + 2,)),
        ],
        cost_estimate=pl.CostEstimate(
            flops=rows * width, bytes_accessed=4 * rows * width, transcendentals=0
        ),
    )(hidden_out, table, queries, positive)
    return hidden_out, embedding, loss.reshape(count)


def solution(mesh):
    in_specs = (
        P("grp", "seq", None),
        P("grp"),
        P(),
        P(),
        P(),
        P(),
        P("grp", None),
        P("grp", None),
        P(),
        P(),
        P("grp", None),
        P("grp"),
    )
    out_specs = (P("grp", "seq", None), P("grp", None), P("grp"))
    sized = functools.partial(body, mesh.shape["seq"], mesh.shape["grp"])
    return jax.shard_map(sized, mesh=mesh, in_specs=in_specs, out_specs=out_specs, check_vma=False)
```

```python
import functools
import math

import jax
import jax.numpy as jnp
from jax import lax
from jax.experimental import pallas as pl
from jax.experimental.pallas import tpu as pltpu
from jax.sharding import PartitionSpec as P

HEAD_DIM = 64
PAIR = 2 * HEAD_DIM
LOW = -1e30
TILE = 256
WIDE = 512
HALVES = 4
STRIPS = 8
MESH = pl.DeviceIdType.MESH
F32 = jnp.float32
BF16 = jnp.bfloat16


def layer_norm(values, gain, shift):
    average = jnp.mean(values, axis=-1, keepdims=True)
    centred = values - average
    variance = jnp.mean(centred * centred, axis=-1, keepdims=True)
    return centred * lax.rsqrt(variance + 1e-05) * gain + shift


def span(index, size):
    return pl.ds(pl.multiple_of(index * size, size), size)


def flip(index, bit):
    step = 1 << bit
    return index + (1 - 2 * ((index // step) % 2)) * step


class Gather:
    def __init__(self, source, held, send, recv, mine, order):
        self.source, self.held, self.send_sem, self.recv_sem = source, held, send, recv
        self.mine, self.order = mine, order
        self.rows = source.shape[0]

    def origin(self, piece, base):
        for place, bit in enumerate(self.order):
            if (piece >> place) & 1:
                base = flip(base, bit)
        return base

    def copy(self, stage, piece, incoming):
        peer = flip(self.mine, self.order[stage])
        owner = self.origin(piece, peer if incoming else self.mine)
        there = self.held.at[span(owner, self.rows)]
        slot = (1 << stage) - 1 + piece
        return pltpu.make_async_remote_copy(
            src_ref=self.source if piece == 0 and not incoming else there,
            dst_ref=there,
            send_sem=self.send_sem.at[slot],
            recv_sem=self.recv_sem.at[slot],
            device_id={"grp": peer},
            device_id_type=MESH,
        )

    def begin(self, stage):
        self.copy(stage, 0, False).start()

    def pass_on(self, stage, piece):
        self.copy(stage, piece, True).wait_recv()
        for later in range(stage + 1, len(self.order)):
            self.copy(later, (1 << stage) + piece, False).start()

    def drain(self):
        for stage in range(len(self.order)):
            for piece in range(1 << stage):
                self.copy(stage, piece, False).wait_send()


def kernel(
    seq_size,
    grp_size,
    tok_hbm,
    length_ref,
    wp_hbm,
    wo_hbm,
    gain1_hbm,
    shift1_hbm,
    up_hbm,
    down_hbm,
    gain2_hbm,
    shift2_hbm,
    out_hbm,
    table_hbm,
    gain1,
    shift1,
    gain2,
    shift2,
    hid,
    wp,
    wo,
    up,
    down,
    qm,
    kbuf,
    vt,
    acc,
    high,
    summed,
    bias,
    scores,
    att,
    normed,
    inner,
    outer,
    final,
    totals,
    embeds,
    local_sem,
    below_send,
    below_recv,
    above_send,
    above_recv,
    up_send,
    up_recv,
    down_send,
    down_recv,
    tot_send,
    tot_recv,
    emb_send,
    emb_recv,
):
    rank = lax.axis_index("seq")
    group = lax.axis_index("grp")
    rows, width = tok_hbm.shape[1:]
    ff = up_hbm.shape[1]
    heads = width // HEAD_DIM
    pairs = width // PAIR
    part = rows // HALVES
    length = length_ref[0]
    bits = grp_size.bit_length() - 1

    barrier = pltpu.get_barrier_semaphore()
    for step in range(1, seq_size):
        pl.semaphore_signal(
            barrier,
            inc=1,
            device_id={"seq": (rank + step) % seq_size},
            device_id_type=MESH,
        )
    for step in range(1, grp_size):
        pl.semaphore_signal(
            barrier,
            inc=1,
            device_id={"grp": (group + step) % grp_size},
            device_id_type=MESH,
        )
    loads = [
        pltpu.make_async_copy(tok_hbm.at[0], hid.at[span(rank, rows)], local_sem.at[0]),
        pltpu.make_async_copy(wp_hbm, wp, local_sem.at[1]),
        pltpu.make_async_copy(wo_hbm, wo, local_sem.at[2]),
        pltpu.make_async_copy(up_hbm, up.at[span(group, up_hbm.shape[0])], local_sem.at[3]),
        pltpu.make_async_copy(down_hbm, down.at[span(group, down_hbm.shape[0])], local_sem.at[4]),
        pltpu.make_async_copy(gain1_hbm, gain1, local_sem.at[5]),
        pltpu.make_async_copy(shift1_hbm, shift1, local_sem.at[6]),
        pltpu.make_async_copy(gain2_hbm, gain2, local_sem.at[7]),
        pltpu.make_async_copy(shift2_hbm, shift2, local_sem.at[8]),
    ]
    pl.semaphore_wait(barrier, seq_size - 1 + grp_size - 1)

    def chain(upward, step, half, incoming, first=False):
        way = 1 if upward else -1
        owner = rank - way * step if incoming else rank - way * (step - 1)
        there = hid.at[span(owner * HALVES + half, part)]
        slot = (step - 1) * HALVES + half
        sends, recvs = (below_send, below_recv) if upward else (above_send, above_recv)
        return pltpu.make_async_remote_copy(
            src_ref=tok_hbm.at[0, pl.ds(half * part, part)] if first else there,
            dst_ref=there,
            send_sem=sends.at[slot],
            recv_sem=recvs.at[slot],
            device_id={"seq": rank + way},
            device_id_type=MESH,
        )

    def has_next(upward):
        return rank + 1 < seq_size if upward else rank >= 1

    def holds(upward, step):
        return rank - step >= 0 if upward else rank + step < seq_size

    for half in range(HALVES):
        for upward in (True, False):

            @pl.when(has_next(upward))
            def _(upward=upward, half=half):
                chain(upward, 1, half, False, True).start()

    for load in loads[:2]:
        load.start()
    order = list(range(1, bits)) + [0]
    back = list(reversed(range(1, bits))) + [0]
    ups = Gather(up_hbm, up, up_send, up_recv, group, order)
    downs = Gather(down_hbm, down, down_send, down_recv, group, back)
    for stage in range(bits):
        ups.begin(stage)
        downs.begin(stage)
    for load in loads[2:]:
        load.start()
    events = [(stage, piece) for stage in range(bits - 1) for piece in range(1 << stage)]
    early, late = events[: seq_size - 2], events[seq_size - 2 :]

    loads[0].wait()
    loads[1].wait()

    factor = math.log2(math.e) / math.sqrt(HEAD_DIM)
    own = span(rank, rows)

    @pl.loop(0, width // TILE, unroll=2)
    def _(tile):
        query = jnp.dot(hid[own, :], wp[:, span(tile, TILE)], preferred_element_type=F32) * factor
        query = query.T.astype(BF16)
        for pair in range(TILE // PAIR):
            at = tile * (TILE // HEAD_DIM) + 2 * pair
            here = pair * PAIR
            blank = jnp.zeros((HEAD_DIM, rows), BF16)
            qm[at] = jnp.concatenate([query[here : here + HEAD_DIM], blank], axis=0)
            qm[at + 1] = jnp.concatenate([blank, query[here + HEAD_DIM : here + PAIR]], axis=0)

    acc[...] = jnp.zeros_like(acc)
    summed[...] = jnp.zeros_like(summed)
    high[...] = jnp.full_like(high, 2 * LOW)
    ones = jnp.ones((16, part), BF16)

    def attend(unit):
        block = span(unit, part)

        @pl.loop(0, width // TILE, unroll=2)
        def _(tile):
            key = jnp.dot(
                hid[block, :],
                wp[:, pl.ds(pl.multiple_of(width + tile * TILE, TILE), TILE)],
                preferred_element_type=F32,
            )
            kbuf[:, span(tile, TILE)] = key.astype(BF16)
            value = jnp.dot(
                hid[block, :],
                wp[:, pl.ds(pl.multiple_of(2 * width + tile * TILE, TILE), TILE)],
                preferred_element_type=F32,
            )
            vt[span(tile, TILE), :] = value.T.astype(BF16)

        position = lax.broadcasted_iota(jnp.int32, (part, PAIR), 0) + unit * part
        bias[...] = jnp.where(position < length, 0.0, LOW)

        def score(pair, place):
            key = kbuf[:, pl.ds(pair * PAIR, PAIR)]
            shift = jnp.concatenate([bias[...]] * (rows // PAIR), axis=1)
            for side in range(2):
                scores[place, side] = shift + jnp.dot(
                    key, qm[2 * pair + side], preferred_element_type=F32
                )

        def weigh(pair, place):
            for side in range(2):
                head = 2 * pair + side
                score_now = scores[place, side]
                old = high[head, 0:1, :]
                top = jnp.maximum(old, jnp.max(score_now, axis=0, keepdims=True))
                expo = jnp.exp2(score_now - top).astype(BF16)
                alpha = jnp.exp2(old - top)
                value = jnp.concatenate([vt[pl.ds(head * HEAD_DIM, HEAD_DIM), :], ones], axis=0)
                got = jnp.dot(value, expo, preferred_element_type=F32)
                mine = pl.ds(head * HEAD_DIM, HEAD_DIM)
                acc[mine, :] = acc[mine, :] * alpha + got[:HEAD_DIM]
                summed[head] = summed[head] * alpha + got[HEAD_DIM : HEAD_DIM + 8]
                high[head] = jnp.broadcast_to(top, (8, rows))

        score(0, 0)
        for pair in range(pairs):
            if pair + 1 < pairs:
                score(pair + 1, (pair + 1) % 2)
            weigh(pair, pair % 2)

    @pl.loop(0, seq_size * HALVES)
    def _(slot):
        step = slot // HALVES
        half = slot % HALVES
        for upward in (True, False):

            @pl.when(jnp.logical_and(step >= 1, holds(upward, step)))
            def _(upward=upward):
                chain(upward, step, half, True).wait_recv()

                @pl.when(has_next(upward))
                def _():
                    chain(upward, step + 1, half, False).start()

        for index, (stage, piece) in enumerate(early):

            @pl.when(slot == (2 + index) * HALVES - 1)
            def _(stage=stage, piece=piece):
                ups.pass_on(stage, piece)
                downs.pass_on(stage, piece)

        @pl.loop(0, 2)
        def _(upper):
            owner = rank - step + 2 * step * upper

            @pl.when((owner >= 0) & (owner < seq_size) & (step + upper >= 1))
            def _():
                attend(owner * HALVES + half)

    for stage, piece in late:
        ups.pass_on(stage, piece)
        downs.pass_on(stage, piece)

    @pl.loop(0, pairs, unroll=4)
    def _(pair):
        total = acc[span(pair, PAIR), :]
        low_part = total[:HEAD_DIM] * (1.0 / summed[2 * pair, 0:1, :])
        high_part = total[HEAD_DIM:] * (1.0 / summed[2 * pair + 1, 0:1, :])
        att[:, span(pair, PAIR)] = jnp.concatenate([low_part, high_part], axis=0).T.astype(BF16)

    loads[2].wait()

    @pl.loop(0, width // WIDE, unroll=2)
    def _(tile):
        here = span(tile, WIDE)
        mixed = jnp.dot(att[...], wo[:, here], preferred_element_type=F32)
        outer[:, here] = mixed + hid[own, here].astype(F32)

    for load in loads[5:]:
        load.wait()
    few = 128

    @pl.loop(0, rows // few, unroll=4)
    def _(index):
        here = span(index, few)
        normed[here, :] = layer_norm(outer[here, :], gain1[...], shift1[...]).astype(BF16)

    loads[3].wait()
    for piece in range(1 << (bits - 1)):
        ups.pass_on(bits - 1, piece)

    @pl.loop(0, ff // WIDE, unroll=4)
    def _(tile):
        here = span(tile, WIDE)
        before = jnp.dot(normed[...], up[:, here], preferred_element_type=F32)
        half = 0.5 * before
        inner[:, here] = (half + half * lax.erf(before * math.sqrt(0.5))).astype(BF16)

    loads[4].wait()
    for piece in range(1 << (bits - 1)):
        downs.pass_on(bits - 1, piece)

    @pl.loop(0, width // WIDE, unroll=2)
    def _(tile):
        here = span(tile, WIDE)
        back_again = lax.dot_general(
            inner[...], down[here, :], (((1,), (1,)), ((), ())), preferred_element_type=F32
        )
        outer[:, here] = back_again + normed[:, here].astype(F32)

    def finish(index, carry):
        here = span(index, few)
        done = layer_norm(outer[here, :], gain2[...], shift2[...])
        final[here, :] = done.astype(BF16)
        position = lax.broadcasted_iota(jnp.int32, (few, 1), 0) + (rank * rows + index * few)
        done = jnp.where(position < length, done, 0.0)
        return carry + jnp.sum(done, axis=0, keepdims=True)

    local_total = lax.fori_loop(
        0, rows // few, finish, jnp.zeros((1, width), F32), unroll=4
    )
    write = pltpu.make_async_copy(final, out_hbm.at[0], local_sem.at[0])
    totals[rank] = local_total

    def spread(ref, axis, mine, size, step, sends, recvs, incoming):
        slot = (mine - step + size) % size if incoming else mine
        return pltpu.make_async_remote_copy(
            src_ref=ref.at[slot],
            dst_ref=ref.at[slot],
            send_sem=sends.at[step - 1],
            recv_sem=recvs.at[step - 1],
            device_id={axis: (mine + step) % size},
            device_id_type=MESH,
        )

    for step in range(1, seq_size):
        spread(totals, "seq", rank, seq_size, step, tot_send, tot_recv, False).start()
    write.start()

    for step in range(1, seq_size):
        spread(totals, "seq", rank, seq_size, step, tot_send, tot_recv, True).wait_recv()
    pooled = totals[0]
    for place in range(1, seq_size):
        pooled = pooled + totals[place]
    pooled = pooled / length.astype(F32)
    embedding = pooled / jnp.sqrt(jnp.sum(pooled * pooled, axis=-1, keepdims=True) + 1e-06)
    embeds[group] = embedding
    for step in range(1, grp_size):
        spread(embeds, "grp", group, grp_size, step, emb_send, emb_recv, False).start()

    for step in range(1, seq_size):
        spread(totals, "seq", rank, seq_size, step, tot_send, tot_recv, False).wait_send()
        for half in range(HALVES):
            for upward in (True, False):

                @pl.when(jnp.logical_and(has_next(upward), holds(upward, step - 1)))
                def _(upward=upward, half=half, step=step):
                    chain(upward, step, half, False, step == 1).wait_send()

    ups.drain()
    downs.drain()

    for step in range(1, grp_size):
        spread(embeds, "grp", group, grp_size, step, emb_send, emb_recv, True).wait_recv()
    keep = pltpu.make_async_copy(embeds, table_hbm, local_sem.at[1])
    keep.start()
    for step in range(1, grp_size):
        spread(embeds, "grp", group, grp_size, step, emb_send, emb_recv, False).wait_send()
    write.wait()
    keep.wait()


def hand_over(hidden, table_hbm, query_hbm, positive_ref, hidden_out, emb_out, loss_out, *held):
    strips, table, asked_ref, short, come, go = held
    strip = strips.shape[0] // STRIPS
    at = lambda index: pl.ds(index * strip, strip)
    group = lax.axis_index("grp")
    legs = [(table_hbm, table), (query_hbm, asked_ref)]
    legs += [(hidden.at[0, at(i)], strips.at[at(i)]) for i in range(STRIPS)]
    comes = [pltpu.make_async_copy(*leg, come.at[i]) for i, leg in enumerate(legs)]
    goes = [(table.at[group], emb_out), (short, loss_out)]
    goes += [(strips.at[at(i)], hidden_out.at[0, at(i)]) for i in range(STRIPS)]
    goes = [pltpu.make_async_copy(*leg, go.at[i]) for i, leg in enumerate(goes)]
    for copy in comes:
        copy.start()
    comes[0].wait()
    comes[1].wait()
    goes[0].start()
    for index in range(STRIPS):
        comes[2 + index].wait()
        goes[2 + index].start()
    asked = asked_ref[...]
    asked = asked / jnp.sqrt(jnp.sum(asked * asked, axis=-1, keepdims=True) + 1e-06)
    asked = asked.astype(BF16).astype(F32)
    count = asked.shape[0]
    row = lax.broadcasted_iota(jnp.int32, (count, 1), 0)
    wanted = jnp.zeros((count, 1), jnp.int32)
    for place in range(count):
        wanted = jnp.where(row == place, positive_ref[place], wanted)
    picked = jnp.zeros((count, 1), F32)
    weight = jnp.zeros((count, 1), F32)
    for place in range(table.shape[0]):
        passage = table[place].astype(BF16).astype(F32)
        logit = 20.0 * jnp.sum(asked * passage, axis=-1, keepdims=True)
        picked = picked + jnp.where(wanted == place, logit, 0.0)
        weight = weight + jnp.exp(logit)
    loss = jnp.log(weight) - picked
    short[...] = jnp.broadcast_to(loss, (count, PAIR)).T[0:1, :]
    goes[1].start()
    for copy in goes:
        copy.wait()


def body(
    seq_size,
    grp_size,
    hidden_in,
    lengths,
    project_weight,
    output_weight,
    first_gain,
    first_shift,
    up_weight,
    down_weight,
    second_gain,
    second_shift,
    queries,
    positive,
):
    rows, width = hidden_in.shape[1:]
    ff = up_weight.shape[1]
    heads = width // HEAD_DIM
    count = queries.shape[0]
    wide = lambda vector: vector.reshape(1, -1)
    smem = pl.BlockSpec(memory_space=pltpu.SMEM)
    hbm = pl.BlockSpec(memory_space=pl.ANY)
    dma = pltpu.SemaphoreType.DMA
    chain_sems = [dma(((seq_size - 1) * HALVES,))] * 4
    pieces = [dma((grp_size - 1,))] * 4
    hidden_out, table = pl.pallas_call(
        functools.partial(kernel, seq_size, grp_size),
        out_shape=[
            jax.ShapeDtypeStruct(hidden_in.shape, BF16),
            jax.ShapeDtypeStruct((grp_size, 1, width), F32),
        ],
        in_specs=[hbm, smem, hbm, hbm, hbm, hbm, hbm, hbm, hbm, hbm],
        out_specs=[hbm, hbm],
        scratch_shapes=[
            *[pltpu.VMEM((1, width), F32)] * 4,
            pltpu.VMEM((seq_size * rows, width), BF16),
            pltpu.VMEM((width, 3 * width), BF16),
            pltpu.VMEM((width, width), BF16),
            pltpu.VMEM((width, ff), BF16),
            pltpu.VMEM((width, ff), BF16),
            pltpu.VMEM((heads, PAIR, rows), BF16),
            pltpu.VMEM((rows // HALVES, width), BF16),
            pltpu.VMEM((width, rows // HALVES), BF16),
            pltpu.VMEM((width, rows), F32),
            pltpu.VMEM((heads, 8, rows), F32),
            pltpu.VMEM((heads, 8, rows), F32),
            pltpu.VMEM((rows // HALVES, PAIR), F32),
            pltpu.VMEM((2, 2, rows // HALVES, rows), F32),
            pltpu.VMEM((rows, width), BF16),
            pltpu.VMEM((rows, width), BF16),
            pltpu.VMEM((rows, ff), BF16),
            pltpu.VMEM((rows, width), F32),
            pltpu.VMEM((rows, width), BF16),
            pltpu.VMEM((seq_size, 1, width), F32),
            pltpu.VMEM((grp_size, 1, width), F32),
            dma((9,)),
            *chain_sems,
            *pieces,
            dma((seq_size - 1,)),
            dma((seq_size - 1,)),
            dma((grp_size - 1,)),
            dma((grp_size - 1,)),
        ],
        compiler_params=pltpu.CompilerParams(
            collective_id=0, has_side_effects=True, vmem_limit_bytes=54 << 20
        ),
        cost_estimate=pl.CostEstimate(
            flops=8 * rows * width * ff, bytes_accessed=16 * width * ff, transcendentals=rows * ff
        ),
    )(
        hidden_in,
        lengths,
        project_weight,
        output_weight,
        wide(first_gain),
        wide(first_shift),
        up_weight,
        down_weight,
        wide(second_gain),
        wide(second_shift),
    )
    hidden_out, embedding, loss = pl.pallas_call(
        hand_over,
        out_shape=[
            jax.ShapeDtypeStruct(hidden_out.shape, BF16),
            jax.ShapeDtypeStruct((1, width), F32),
            jax.ShapeDtypeStruct((1, count), F32),
        ],
        in_specs=[hbm, hbm, hbm, smem],
        out_specs=[hbm, hbm, hbm],
        scratch_shapes=[
            pltpu.VMEM((rows, width), BF16),
            pltpu.VMEM(table.shape, F32),
            pltpu.VMEM((count, width), F32),
            pltpu.VMEM((1, count), F32),
            dma((STRIPS + 2,)),
            dma((STRIPS + 2,)),
        ],
        cost_estimate=pl.CostEstimate(
            flops=rows * width, bytes_accessed=4 * rows * width, transcendentals=0
        ),
    )(hidden_out, table, queries, positive)
    return hidden_out, embedding, loss.reshape(count)


def solution(mesh):
    in_specs = (
        P("grp", "seq", None),
        P("grp"),
        P(),
        P(),
        P(),
        P(),
        P("grp", None),
        P("grp", None),
        P(),
        P(),
        P("grp", None),
        P("grp"),
    )
    out_specs = (P("grp", "seq", None), P("grp", None), P("grp"))
    sized = functools.partial(body, mesh.shape["seq"], mesh.shape["grp"])
    return jax.shard_map(sized, mesh=mesh, in_specs=in_specs, out_specs=out_specs, check_vma=False)
```
